32 devices in a mesh: band: 8 (over y, x, core), col: 4 (over z).
Axes of the slice: x: 2, y: 2, z: 4, core: 2. Of those that a mesh axis runs over, the one named last changes fastest.
Arguments:
- bands: float32 [4096, 8192], P(('band', 'col')), may hold values from -6 to 6
- row_interp: float32 [8, 512, 640], P('band'), may hold values from -0.25 to 0.25
- col_interp: float32 [16, 640, 512], P('col'), may hold values from -0.25 to 0.25
- row_start: int32 [8], P('band'), may hold values from 0 to 128
- col_start: int32 [16], P('col'), may hold values from 0 to 128
- spacing: float32 [8], P('band'), may hold values from 0.5 to 2
Outputs:
- elevation: float32 [4096, 8192], P('band', 'col')
- slope_sine: float32 [4096, 8192], P('band', 'col')
- hillshade: float32 [4096, 8192], P('band', 'col')
The draws below stay inside these ranges and needn't reach their ends.
All inputs are finite; a program needn't handle non-finite values.
Results may differ from the reference program's by a relative error of at most 0.0003.
Values sent between devices are 32-bit elements; how exact they have to be, the bound alone decides.
No kernel may reach another device: no remote copies, remote signals or barrier semaphores. Data moves between devices by JAX's collectives and lax.ppermute only.
A program may use at most 128 MiB of HBM per device.

```python
import math
import jax
import jax.numpy as jnp
from jax import lax

TILE = 512
MARGIN = 128
WIN = 640
TROWS = 8
TCOLS = 16
ROWS = 4096
COLS = 8192


def place_ends(entries, rng, least, high):
    extent = entries.shape
    spot = [jax.random.randint(jax.random.fold_in(rng, axis), (), 0, extent[axis]) for axis in range(len(extent))]
    entries = entries.at[tuple(spot)].set(least)
    longest = extent.index(max(extent))
    spot[longest] = (spot[longest] + 1) % extent[longest]
    return entries.at[tuple(spot)].set(high)


def level_of(own_key, extent, shards, least, largest):
    factor_of = 1.0
    for dim, shards_of in shards:
        draws = jax.random.uniform(jax.random.fold_in(jax.random.fold_in(own_key, 6), dim), (shards_of,), jnp.float32, least / len(shards), largest / len(shards))
        factor_of = factor_of * jnp.repeat(jnp.exp(draws), extent[dim] // shards_of).reshape((-1,) + (1,) * (len(extent) - 1 - dim))
    return factor_of


def centred(key, dims, scale, bound, cuts=(), held_as=jnp.bfloat16):
    result = scale * jax.random.normal(key, dims, jnp.float32)
    if cuts:
        result = result * level_of(key, dims, cuts, -0.22, 0.18)
    return jnp.clip(result, -bound, bound).astype(held_as)


def setup_inputs(seed: int = 0) -> dict:
    splits = jax.random.split(jax.random.key(seed), 7)
    return {
        "bands": centred(splits[0], (ROWS, COLS), 1.0, 6.0, ((0, 32),), jnp.float32),
        "row_interp": centred(splits[1], (TROWS, TILE, WIN), WIN ** -0.5, 0.25, ((0, 8),), jnp.float32),
        "col_interp": centred(splits[2], (TCOLS, WIN, TILE), WIN ** -0.5, 0.25, ((0, 4),), jnp.float32),
        "row_start": place_ends(jax.random.randint(splits[3], (TROWS,), 0, TILE + 2 * MARGIN - WIN + 1), jax.random.fold_in(splits[3], 1), 0, TILE + 2 * MARGIN - WIN).astype(jnp.int32),
        "col_start": place_ends(jax.random.randint(splits[4], (TCOLS,), 0, TILE + 2 * MARGIN - WIN + 1), jax.random.fold_in(splits[4], 1), 0, TILE + 2 * MARGIN - WIN).astype(jnp.int32),
        "spacing": jnp.clip(jnp.exp(math.log(2.0) - 1.3862944 * jax.random.uniform(splits[5], (TROWS,), jnp.float32) ** level_of(splits[5], (TROWS,), ((0, 8),), -0.2, 0.2)), 0.5, 2.0),
    }


def horn(elevation, spacing):
    z = jnp.pad(elevation, 1)
    scale = 8.0 * jnp.repeat(spacing, TILE)[:, None]
    right = z[:-2, 2:] + 2.0 * z[1:-1, 2:] + z[2:, 2:]
    left = z[:-2, :-2] + 2.0 * z[1:-1, :-2] + z[2:, :-2]
    lower = z[2:, :-2] + 2.0 * z[2:, 1:-1] + z[2:, 2:]
    upper = z[:-2, :-2] + 2.0 * z[:-2, 1:-1] + z[:-2, 2:]
    grad_p = (right - left) / scale
    grad_q = (lower - upper) / scale
    total = grad_p * grad_p + grad_q * grad_q
    denom = jnp.sqrt(1.0 + total)
    slope_sine = jnp.sqrt(total) / denom
    hillshade = (0.70710678 - 0.5 * grad_p + 0.5 * grad_q) / denom
    return (slope_sine, hillshade)

def reference(bands, row_interp, col_interp, row_start, col_start, spacing):
    padded = jnp.pad(bands, MARGIN)
    tcount = col_interp.shape[0]

    def one_row(index):
        start = (index * TILE + row_start[index]).astype(jnp.int32)
        window = lax.dynamic_slice_in_dim(padded, start, WIN, 0)
        rowres = jnp.dot(row_interp[index], window, precision=lax.Precision.HIGHEST, preferred_element_type=jnp.float32)

        def one_col(jindex):
            cstart = (jindex * TILE + col_start[jindex]).astype(jnp.int32)
            cols = lax.dynamic_slice_in_dim(rowres, cstart, WIN, 1)
            return jnp.dot(cols, col_interp[jindex], precision=lax.Precision.HIGHEST, preferred_element_type=jnp.float32)
        tiles = lax.map(one_col, jnp.arange(tcount, dtype=jnp.int32))
        return jnp.moveaxis(tiles, 0, 1).reshape(TILE, tcount * TILE)
    elevation = lax.map(one_row, jnp.arange(row_interp.shape[0], dtype=jnp.int32))
    elevation = elevation.reshape(row_interp.shape[0] * TILE, tcount * TILE)
    slope_sine, hillshade = horn(elevation, spacing)
    return (elevation, slope_sine, hillshade)
```

```python
import functools

import jax
import jax.numpy as jnp
from jax import lax
from jax.experimental import pallas as pl
from jax.experimental.pallas import tpu as pltpu
from jax.sharding import PartitionSpec as P

MARGIN = 128


VMEM = pltpu.VMEM
SMEM = pltpu.SMEM


def split(x):
    high = x.astype(jnp.bfloat16)
    return high, (x - high.astype(jnp.float32)).astype(jnp.bfloat16)


def dot3(a, b):
    (ah, al), (bh, bl) = a, b
    dot = functools.partial(jnp.dot, preferred_element_type=jnp.float32)
    return dot(ah, bh) + (dot(ah, bl) + dot(al, bh))


def shifted_rows_kernel(start, x_ref, high_ref, low_ref):
    width = high_ref.shape[1]
    x = x_ref[0]
    x = jnp.concatenate([x, jnp.zeros((x.shape[0], width - x.shape[1]), x.dtype)], 1)
    high_ref[...], low_ref[...] = split(pltpu.roll(x, start[0], 1))


def shifted_cols_kernel(start, x_ref, high_ref, low_ref):
    depth = high_ref.shape[1]
    x = x_ref[0]
    x = jnp.concatenate([x, jnp.zeros((depth - x.shape[0], x.shape[1]), x.dtype)], 0)
    high_ref[0], low_ref[0] = split(pltpu.roll(x, start[pl.program_id(0)], 0))


def pad_row_interp(row_interp, row_start, depth):
    _, tile, width = row_interp.shape
    shape = jax.ShapeDtypeStruct((tile, depth), jnp.bfloat16)
    return pl.pallas_call(
        shifted_rows_kernel,
        out_shape=(shape, shape),
        in_specs=[pl.BlockSpec(memory_space=SMEM), pl.BlockSpec(memory_space=VMEM)],
        out_specs=(pl.BlockSpec(memory_space=VMEM),) * 2,
        name="pad_row_interp",
    )(row_start, row_interp)


def pad_col_interp(col_interp, col_start, depth):
    count, width, tile = col_interp.shape
    shape = jax.ShapeDtypeStruct((count, depth, tile), jnp.bfloat16)
    block = pl.BlockSpec((1, depth, tile), lambda i: (i, 0, 0))
    return pl.pallas_call(
        shifted_cols_kernel,
        grid=(count,),
        out_shape=(shape, shape),
        in_specs=[
            pl.BlockSpec(memory_space=SMEM),
            pl.BlockSpec((1, width, tile), lambda i: (i, 0, 0)),
        ],
        out_specs=(block, block),
        name="pad_col_interp",
    )(col_start, col_interp)


def rows_of_chunk(places, slots, top, bottom, high, low):
    margin, rows = top.shape[0], slots[0].shape[0]
    depth = high.shape[0]
    high[0:margin, :], low[0:margin, :] = split(top[...])
    high[depth - margin : depth, :], low[depth - margin : depth, :] = split(bottom[...])
    for k, slot in enumerate(slots):
        spot = pl.ds(pl.multiple_of(margin + places[k] * rows, rows), rows)
        high[spot, :], low[spot, :] = split(slot[...])


def edge_kernel(n, places, *refs):
    slots, (top, bottom, rh, rl, out_h, out_l, first, last, xh, xl) = refs[:n], refs[n:]
    rows_of_chunk(places, slots, top, bottom, xh, xl)
    rr = dot3((rh[...], rl[...]), (xh[...], xl[...]))
    margin = first.shape[1]
    first[...], last[...] = rr[:, :margin], rr[:, margin:]
    out_h[...], out_l[...] = split(rr)


def tile_kernel(n, parts, sides, aliased, places, *refs):
    slots, refs = refs[:n], refs[n:]
    top, bottom, rh, rl, ch, cl = refs[:6]
    refs = refs[6:]
    olds = 1 + max([p[1] for p in parts if p[0] == "old"], default=-1)
    wides = 1 + max([p[1] for p in parts if p[0] == "wide"], default=-1)
    old, refs = refs[: 2 * olds], refs[2 * olds :]
    wide, refs = refs[:wides], refs[wides:]
    if aliased:
        refs = refs[1:]
    elev, out_h, out_l, head, tail = refs[:5]
    refs = refs[5:]
    side, (xh, xl) = refs[:-2], refs[-2:]
    rows_of_chunk(places, slots, top, bottom, xh, xl)
    new = split(dot3((rh[...], rl[...]), (xh[...], xl[...])))
    out_h[...], out_l[...] = new
    window = ([], [])
    for part in parts:
        if part[0] == "new":
            pair = tuple(v[:, part[1] : part[2]] for v in new)
        elif part[0] == "old":
            pair = tuple(v[:, part[2] : part[3]] for v in old[2 * part[1] : 2 * part[1] + 2])
        else:
            pair = split(wide[part[1]][...])
        window[0].append(pair[0])
        window[1].append(pair[1])
    window = tuple(jnp.concatenate(w, 1) for w in window)
    z = dot3(window, (ch[0], cl[0]))
    elev[...] = z
    head[...] = z[:8]
    tail[...] = z[z.shape[0] - 8 :]
    for ref, where in zip(side, sides):
        lanes = z[:, :128] if where == "first" else z[:, z.shape[1] - 128 :]
        flipped = lanes.T
        ref[...] = flipped[:8] if where == "first" else flipped[120:]


def horn_kernel(count, inverse, *refs):
    z, refs = refs[0], refs[1:]
    tops, bottoms, refs = refs[:count], refs[count : 2 * count], refs[2 * count :]
    left_s, left_d, right_s, right_d, slope, shade = refs
    strips = z.shape[0] // 8
    width = z.shape[1]
    here = slope.shape[0] // 8
    step = pl.program_id(0)
    scale = inverse[0]
    row = lax.broadcasted_iota(jnp.int32, (8, width), 0)
    col = lax.broadcasted_iota(jnp.int32, (8, width), 1)
    top = jnp.concatenate([t[...] for t in tops], 1)
    bottom = jnp.concatenate([t[...] for t in bottoms], 1)

    def strip(r, carry):
        g = step * here + r
        spot = lambda s: pl.ds(pl.multiple_of(s * 8, 8), 8)
        now = z[spot(g), :]
        above = jnp.where(g == 0, top, z[spot(jnp.maximum(g - 1, 0)), :])
        below = jnp.where(g == strips - 1, bottom, z[spot(jnp.minimum(g + 1, strips - 1)), :])
        up = jnp.where(row == 0, pltpu.roll(above, 1, 0), pltpu.roll(now, 1, 0))
        down = jnp.where(row == 7, pltpu.roll(below, 7, 0), pltpu.roll(now, 7, 0))
        s = up + 2.0 * now + down
        d = down - up
        ls, ld = left_s[spot(g), :][:, :1], left_d[spot(g), :][:, :1]
        gs, gd = right_s[spot(g), :][:, :1], right_d[spot(g), :][:, :1]
        s_left = jnp.where(col == 0, ls, pltpu.roll(s, 1, 1))
        s_right = jnp.where(col == width - 1, gs, pltpu.roll(s, width - 1, 1))
        d_left = jnp.where(col == 0, ld, pltpu.roll(d, 1, 1))
        d_right = jnp.where(col == width - 1, gd, pltpu.roll(d, width - 1, 1))
        p = (s_right - s_left) * scale
        q = (d_left + 2.0 * d + d_right) * scale
        total = p * p + q * q
        inv = lax.rsqrt(1.0 + total)
        slope[spot(r), :] = jnp.sqrt(total) * inv
        shade[spot(r), :] = (0.70710678 - 0.5 * p + 0.5 * q) * inv
        return carry

    lax.fori_loop(0, here, strip, 0)


def on_device(bands, row_interp, col_interp, row_start, col_start, spacing):
    n = lax.axis_size("col")
    nb = lax.axis_size("band")
    me = lax.axis_index("col")
    margin = MARGIN
    rows = bands.shape[0]
    width = bands.shape[1] // n
    tile = row_interp.shape[1]
    count = col_interp.shape[0]
    depth = tile + 2 * margin
    f32, bf16 = jnp.float32, jnp.bfloat16

    xor = n & (n - 1) == 0
    peer = (lambda i, k: i ^ k) if xor else (lambda i, k: (i + k) % n)
    source = (lambda i, k: i ^ k) if xor else (lambda i, k: (i - k) % n)
    places = jnp.stack([source(me, k) for k in range(n)]).astype(jnp.int32)
    up = [(i, i + 1) for i in range(nb - 1)]
    down = [(i + 1, i) for i in range(nb - 1)]
    right = [(i, i + 1) for i in range(n - 1)]
    left = [(i + 1, i) for i in range(n - 1)]

    order = [0, count - 1] + list(range(1, count - 1))
    chunks = [[(0, margin), (width - margin, width)]]
    done = [(0, margin), (width - margin, width)]
    for t in order:
        low, high = max(t * tile - margin, 0), min((t + 1) * tile + margin, width)
        free = [i for i in range(low, high, margin) if not any(a <= i < b for a, b in done)]
        chunks.append([(free[0], free[-1] + margin)])
        done.append(chunks[-1][0])

    def cut(chunk, owner):
        return jnp.concatenate(
            [lax.dynamic_slice(bands, (0, owner * width + a), (rows, b - a)) for a, b in chunk], 1
        )

    slots = []
    for chunk in chunks:
        got = [cut(chunk, me)]
        for k in range(n - 1, 0, -1):
            pairs = [(i, peer(i, k)) for i in range(n)]
            got.insert(1, lax.ppermute(cut(chunk, peer(me, k)), "col", pairs))
        slots.append(got)

    def rows_from(got, sources, last):
        pieces = []
        for s in sources:
            slot = source(me, s) if xor else (me - s) % n
            block = got[0]
            for k in range(1, n):
                block = jnp.where(slot == k, got[k], block)
            if rows > margin:
                block = block[rows - margin :] if last else block[:margin]
            pieces.append(block)
        return pieces[0] if len(pieces) == 1 else jnp.concatenate(pieces, 0)

    many = max(margin // rows, 1)
    tops, bottoms = [], []
    for got in slots:
        tops.append(lax.ppermute(rows_from(got, range(n - many, n), True), "band", up))
        bottoms.append(lax.ppermute(rows_from(got, range(many), False), "band", down))

    rh, rl = pad_row_interp(row_interp, row_start, depth)
    ch, cl = pad_col_interp(col_interp, col_start, depth)

    vm = pl.BlockSpec(memory_space=VMEM)
    sm = pl.BlockSpec(memory_space=SMEM)
    anywhere = pl.BlockSpec(memory_space=pl.ANY)

    def wide_of(chunk):
        return sum(b - a for a, b in chunk)

    w = wide_of(chunks[0])
    eh, el, first, last = pl.pallas_call(
        functools.partial(edge_kernel, n),
        out_shape=(
            jax.ShapeDtypeStruct((tile, w), bf16),
            jax.ShapeDtypeStruct((tile, w), bf16),
            jax.ShapeDtypeStruct((tile, margin), f32),
            jax.ShapeDtypeStruct((tile, margin), f32),
        ),
        in_specs=[sm] + [vm] * (n + 4),
        out_specs=(vm,) * 4,
        scratch_shapes=[pltpu.VMEM((depth, w), bf16)] * 2,
        name="edge_rows",
    )(places, *slots[0], tops[0], bottoms[0], rh, rl)
    from_left = lax.ppermute(last, "col", right)
    from_right = lax.ppermute(first, "col", left)

    spans = [(0, margin, 0, 0), (width - margin, width, 0, margin)]
    rr = [(eh, el)]
    elev = None
    heads, tails, sides = {}, {}, {}
    for index, t in enumerate(order, 1):
        chunk = chunks[index]
        a0, b0 = chunk[0]
        w = wide_of(chunk)
        parts, olds, wides = [], [], []
        low, high = t * tile - margin, (t + 1) * tile + margin
        at = low
        while at < high:
            if at < 0 or at >= width:
                wides.append(from_left if at < 0 else from_right)
                parts.append(("wide", len(wides) - 1))
                at += margin
            elif a0 <= at < b0:
                end = min(b0, high)
                parts.append(("new", at - a0, end - a0))
                at = end
            else:
                a, b, which, base = [s for s in spans if s[0] <= at < s[1]][0]
                end = min(b, high)
                if which not in olds:
                    olds.append(which)
                parts.append(("old", olds.index(which), at - a + base, end - a + base))
                at = end
        side = [s for s, here in (("first", t == 0), ("last", t == count - 1)) if here]
        operands = [places, *slots[index], tops[index], bottoms[index], rh, rl, ch, cl]
        specs = [sm] + [vm] * (n + 4) + [pl.BlockSpec((1, depth, tile), lambda i, t=t: (t, 0, 0))] * 2
        for which in olds:
            operands += rr[which]
            specs += [vm] * 2
        operands += wides
        specs += [vm] * len(wides)
        alias = {}
        if elev is not None:
            alias = {len(operands): 0}
            operands.append(elev)
            specs.append(anywhere)
        out = pl.pallas_call(
            functools.partial(tile_kernel, n, tuple(parts), tuple(side), bool(alias)),
            out_shape=(
                jax.ShapeDtypeStruct((tile, width), f32),
                jax.ShapeDtypeStruct((tile, w), bf16),
                jax.ShapeDtypeStruct((tile, w), bf16),
                jax.ShapeDtypeStruct((8, tile), f32),
                jax.ShapeDtypeStruct((8, tile), f32),
            )
            + (jax.ShapeDtypeStruct((8, tile), f32),) * len(side),
            grid=(1,),
            in_specs=specs,
            out_specs=(pl.BlockSpec((tile, tile), lambda i, t=t: (0, t)),) + (vm,) * (4 + len(side)),
            scratch_shapes=[pltpu.VMEM((depth, w), bf16)] * 2,
            input_output_aliases=alias,
            name=f"tile_{t}",
        )(*operands)
        elev = out[0]
        rr.append((out[1], out[2]))
        spans.append((a0, b0, index, 0))
        tails[t] = lax.ppermute(out[4], "band", up)
        heads[t] = lax.ppermute(out[3], "band", down)
        for s, v in zip(side, out[5:]):
            sides[s] = v

    line = jnp.concatenate([tails[0][7, :1], sides["first"][0], heads[0][0, :1]])
    right_line = lax.ppermute(line, "col", left)
    end = count - 1
    line = jnp.concatenate([tails[end][7, -1:], sides["last"][7], heads[end][0, -1:]])
    left_line = lax.ppermute(line, "col", right)

    def across(v):
        smooth = v[:-2] + 2.0 * v[1:-1] + v[2:]
        steep = v[2:] - v[:-2]
        return tuple(jnp.broadcast_to(x[:, None], (tile, 128)) for x in (smooth, steep))

    strip = min(64, tile)
    whole = pl.BlockSpec((tile, width), lambda i: (0, 0))
    small = pl.BlockSpec((8, tile), lambda i: (0, 0))
    lane = pl.BlockSpec((tile, 128), lambda i: (0, 0))
    block = pl.BlockSpec((strip, width), lambda i: (i, 0))
    shape = jax.ShapeDtypeStruct((tile, width), f32)
    slope, shade = pl.pallas_call(
        functools.partial(horn_kernel, count),
        grid=(tile // strip,),
        out_shape=(shape, shape),
        in_specs=[sm, whole] + [small] * (2 * count) + [lane] * 4,
        out_specs=(block, block),
        name="horn",
    )(
        0.125 / spacing,
        elev,
        *[tails[t] for t in range(count)],
        *[heads[t] for t in range(count)],
        *across(left_line),
        *across(right_line),
    )
    return (elev, slope, shade)


def solution(mesh):
    in_specs = (
        P(("band", "col"), None),
        P("band", None, None),
        P("col", None, None),
        P("band"),
        P("col"),
        P("band"),
    )
    out_specs = (P("band", "col"), P("band", "col"), P("band", "col"))
    return jax.shard_map(
        on_device, mesh=mesh, in_specs=in_specs, out_specs=out_specs, check_vma=False
    )
```

```python
import functools

import jax
import jax.numpy as jnp
from jax import lax
from jax.experimental import pallas as pl
from jax.experimental.pallas import tpu as pltpu
from jax.sharding import PartitionSpec as P


MARGIN = 128


VMEM = pltpu.VMEM
SMEM = pltpu.SMEM


def split(x):
    high = x.astype(jnp.bfloat16)
    return high, (x - high.astype(jnp.float32)).astype(jnp.bfloat16)


def dot3(a, b):
    (ah, al), (bh, bl) = a, b
    dot = functools.partial(jnp.dot, preferred_element_type=jnp.float32)
    return dot(ah, bh) + (dot(ah, bl) + dot(al, bh))


def params(mib):
    return pltpu.CompilerParams(vmem_limit_bytes=mib << 20)


def shifted_rows_kernel(start, x_ref, high_ref, low_ref):
    width = high_ref.shape[1]
    x = x_ref[0]
    x = jnp.concatenate([x, jnp.zeros((x.shape[0], width - x.shape[1]), x.dtype)], 1)
    high_ref[...], low_ref[...] = split(pltpu.roll(x, start[0], 1))


def shifted_cols_kernel(start, x_ref, high_ref, low_ref):
    count, depth, tile = high_ref.shape
    for t in range(count):
        x = x_ref[t]
        x = jnp.concatenate([x, jnp.zeros((depth - x.shape[0], tile), x.dtype)], 0)
        high_ref[t], low_ref[t] = split(pltpu.roll(x, start[t], 0))


def pad_interp(kernel, start, x, shape):
    return pl.pallas_call(
        kernel,
        out_shape=(VMEM(shape, jnp.bfloat16),) * 2,
        in_specs=[pl.BlockSpec(memory_space=SMEM), pl.BlockSpec(memory_space=VMEM)],
        out_specs=(pl.BlockSpec(memory_space=VMEM),) * 2,
        compiler_params=params(16),
    )(start, x)


def peer(i, k, n):
    return i ^ k if n & (n - 1) == 0 else (i + k) % n


def source(i, k, n):
    return i ^ k if n & (n - 1) == 0 else (i + n - k) % n


def pack_kernel(n, jobs, bands, *outs):
    me = lax.axis_index("col")
    total = bands.shape[1]
    for (k, first), out in zip(jobs, outs):
        wide = out.shape[1]
        start = jnp.clip(peer(me, k, n) * (total // n) + first, 0, total - wide)
        out[...] = bands[:, pl.ds(pl.multiple_of(start, 128), wide)]


def select_kernel(n, margin, *refs):
    slots, outs = refs[:n], refs[n:]
    me = lax.axis_index("col")
    rows = slots[0].shape[0]
    part = min(rows, margin)
    many = margin // part
    for out, owners, inner in ((outs[0], n - many, rows - part), (outs[1], 0, 0)):
        for j in range(many):
            for k in range(n):

                @pl.when(source(me, k, n) == owners + j)
                def _():
                    out[j * part : (j + 1) * part, :] = slots[k][inner : inner + part, :]


def lines_kernel(first, last, tops, bottoms, to_left, to_right):
    tile, wide = first.shape[1], tops.shape[1]
    to_left[:, :tile] = first[0:1, :]
    to_left[:, tile : tile + 128] = tops[7:8, :128]
    to_left[:, tile + 128 :] = bottoms[0:1, :128]
    to_right[:, :tile] = last[7:8, :]
    to_right[:, tile : tile + 128] = tops[7:8, wide - 128 :]
    to_right[:, tile + 128 :] = bottoms[0:1, wide - 128 :]


def tile_kernel(n, margin, t, parts, sides, doubled, held, *refs):
    slots, refs = refs[:n], refs[n:]
    others, refs = refs[: (n - 1) * doubled], refs[(n - 1) * doubled :]
    top, bottom, rh, rl, ch, cl = refs[:6]
    refs = refs[6:]
    olds = 1 + max([p[1] for p in parts if p[0] == "old"], default=-1)
    old, refs = refs[: 2 * olds], refs[2 * olds :]
    before, refs = refs[: 2 * held], refs[2 * held :]
    z, head, tail, out_h, out_l = refs[:5]
    refs = refs[5:]
    side, (high, low) = refs[:-2], refs[-2:]
    me = lax.axis_index("col")
    rows = slots[0].shape[0]
    depth = high.shape[0]
    high[0:margin, :], low[0:margin, :] = split(top[...])
    high[depth - margin : depth, :], low[depth - margin : depth, :] = split(bottom[...])
    for k, slot in enumerate(slots):
        spot = pl.ds(pl.multiple_of(margin + source(me, k, n) * rows, rows), rows)
        x = slot[...]
        if doubled and k:
            x = x + others[k - 1][...]
        high[spot, :], low[spot, :] = split(x)
    rr = dot3((rh[...], rl[...]), (high[...], low[...]))
    none = jnp.zeros((rr.shape[0], margin), rr.dtype)
    if "first" in sides:
        rr = jnp.where(me == 0, jnp.concatenate([none, rr[:, :-margin]], 1), rr)
    if "last" in sides:
        rr = jnp.where(me == n - 1, jnp.concatenate([rr[:, margin:], none], 1), rr)
    new = split(rr)
    out_h[...], out_l[...] = new
    window = ([], [])
    for part in parts:
        if part[0] == "new":
            pair = tuple(v[:, part[1] : part[2]] for v in new)
        else:
            pair = tuple(v[:, part[2] : part[3]] for v in old[2 * part[1] : 2 * part[1] + 2])
        window[0].append(pair[0])
        window[1].append(pair[1])
    window = tuple(jnp.concatenate(w, 1) for w in window)
    value = dot3(window, (ch[t], cl[t]))
    z[...] = value
    tile = value.shape[1]
    at = head.shape[1] - tile
    if held:
        head[:, :at], tail[:, :at] = before[0][...], before[1][...]
    head[:, at:] = value[:8]
    tail[:, at:] = value[value.shape[0] - 8 :]
    for ref, where in zip(side, sides):
        lanes = value[:, :128] if where == "first" else value[:, tile - 128 :]
        flipped = lanes.T
        ref[...] = flipped[:8] if where == "first" else flipped[120:]


def horn(up, now, down, scale):
    width = now.shape[1]
    s = up + 2.0 * now + down
    d = down - up
    before = lambda v: pltpu.roll(v, 1, 1)[:, 128 : width - 128]
    after = lambda v: pltpu.roll(v, width - 1, 1)[:, 128 : width - 128]
    p = (after(s) - before(s)) * scale
    q = (before(d) + 2.0 * d[:, 128 : width - 128] + after(d)) * scale
    total = p * p + q * q
    inv = lax.rsqrt(1.0 + total)
    root = total * lax.rsqrt(jnp.maximum(total, 1.2e-38))
    return root * inv, (0.70710678 - 0.5 * p + 0.5 * q) * inv


def upright(line, rows):
    return jnp.broadcast_to(line, (128, rows)).T


def cut(tiles, rows, first, last, ends):
    tile = tiles[0].shape[1]
    width = tile * len(tiles)
    pieces = [ends[0]] if first < 0 else []
    at = max(first, 0)
    while at < min(last, width):
        t, stop = at // tile, min(at // tile * tile + tile, last)
        pieces.append(tiles[t][rows, at - t * tile : stop - t * tile])
        at = stop
    if last > width:
        pieces.append(ends[1])
    return jnp.concatenate(pieces, 1)


def horn_kernel(count, ranges, fresh, held, spacing, *refs):
    tiles, (left, right) = refs[:count], refs[count : count + 2]
    elev, slope, shade, *bufs, l_col, r_col, sem_z, sem_out = refs[count + 2 + held :]
    tile = tiles[0].shape[0]
    width = tile * count
    blocks = 4 if tile % 32 == 0 else 1
    rows = tile // blocks

    def keep(j):
        return pltpu.make_async_copy(
            tiles[fresh[j]], elev.at[:, pl.ds(fresh[j] * tile, tile)], sem_z.at[j]
        )

    def store(i, b, which):
        first, last = ranges[i]
        return pltpu.make_async_copy(
            bufs[2 * i + which].at[pl.ds(b * rows, rows), :],
            (slope, shade)[which].at[pl.ds(b * rows, rows), pl.ds(first, last - first)],
            sem_out.at[i, b, which],
        )

    for j in range(len(fresh)):
        keep(j).start()
    if any(first == 0 for first, _ in ranges):
        l_col[...] = upright(left[0:1, :tile], tile)
    if any(last == width for _, last in ranges):
        r_col[...] = upright(right[0:1, :tile], tile)
    strips = tile // 8
    for i, (first, last) in enumerate(ranges):
        pieces, at = [], first
        while at < last:
            pieces.append((at, min(at + 384, last)))
            at = pieces[-1][1]
        for b in range(blocks):
            for lo, hi in pieces:
                row = lax.broadcasted_iota(jnp.int32, (8, hi - lo + 256), 0)
                scale = 0.125 / jnp.full((8, hi - lo), spacing[0])

                def load(g):
                    spot = pl.ds(pl.multiple_of(g * 8, 8), 8)
                    ends = (l_col[spot, :], r_col[spot, :])
                    return cut(tiles, spot, lo - 128, hi + 128, ends)

                def strip(r, carry):
                    g = b * (rows // 8) + r
                    before, above = carry
                    now = load(g)
                    below = load(jnp.minimum(g + 1, strips - 1))
                    rolled = pltpu.roll(now, 1, 0)
                    ahead = pltpu.roll(below, 7, 0)
                    up = jnp.where(row == 0, before, rolled)
                    down = jnp.where(row == 7, ahead, above)
                    spot = pl.ds(pl.multiple_of(g * 8, 8), 8)
                    where = pl.ds(lo - first, hi - lo)
                    bufs[2 * i][spot, where], bufs[2 * i + 1][spot, where] = horn(up, now, down, scale)
                    return rolled, ahead

                g0 = b * (rows // 8)
                start = (pltpu.roll(load(max(g0 - 1, 0)), 1, 0), pltpu.roll(load(g0), 7, 0))
                lax.fori_loop(0, rows // 8, strip, start, unroll=8)
            store(i, b, 0).start()
            store(i, b, 1).start()
    for i in range(len(ranges)):
        for b in range(blocks):
            store(i, b, 0).wait()
            store(i, b, 1).wait()
    for j in range(len(fresh)):
        keep(j).wait()


def border_kernel(count, slices, spacing, *refs):
    tiles, (left, right), refs = refs[:count], refs[count : count + 2], refs[count + 2 :]
    tops, bottoms = refs[:2], refs[2:4]
    slope, shade, buf, sem = refs[-4:]
    tile = tiles[0].shape[0]
    width = tile * count
    row = lax.broadcasted_iota(jnp.int32, (8, width + 256), 0)
    scale = 0.125 / jnp.full((8, width), spacing[0])

    def halo(groups, at):
        inner = [groups[g][at : at + 1, tile * j : tile * (j + 1)] for g, j in slices]
        side = tile if at == 7 else tile + 128
        ends = [v[0:1, side : side + 128] for v in (left, right)]
        return jnp.broadcast_to(jnp.concatenate([ends[0]] + inner + [ends[1]], 1), row.shape)

    def strip(at):
        lane = at // 128 * 128
        ends = [upright(v[0:1, lane : lane + 128], 128)[at - lane : at - lane + 8] for v in (left, right)]
        return cut(tiles, slice(at, at + 8), -128, width + 128, ends)

    copies = []
    for where, at in enumerate((0, tile - 8)):
        now = strip(at)
        above = halo(tops, 7) if where == 0 else pltpu.roll(strip(at - 8), 1, 0)
        below = halo(bottoms, 0) if where == 1 else pltpu.roll(strip(8), 7, 0)
        up = jnp.where(row == 0, above, pltpu.roll(now, 1, 0))
        down = jnp.where(row == 7, below, pltpu.roll(now, 7, 0))
        for j, (v, out) in enumerate(zip(horn(up, now, down, scale), (slope, shade))):
            buf[where, j] = v
            copies.append(
                pltpu.make_async_copy(buf.at[where, j], out.at[pl.ds(at, 8), :], sem.at[where, j])
            )
            copies[-1].start()
    for copy in copies:
        copy.wait()


def on_device(bands, row_interp, col_interp, row_start, col_start, spacing):
    n = lax.axis_size("col")
    nb = lax.axis_size("band")
    margin = MARGIN
    rows, total = bands.shape
    width = total // n
    tile = row_interp.shape[1]
    count = col_interp.shape[0]
    depth = tile + 2 * margin
    f32, bf16 = jnp.float32, jnp.bfloat16
    vm = pl.BlockSpec(memory_space=VMEM)
    sm = pl.BlockSpec(memory_space=SMEM)
    hbm = pl.BlockSpec(memory_space=pltpu.HBM)

    up = [(i, i + 1) for i in range(nb - 1)]
    down = [(i + 1, i) for i in range(nb - 1)]
    right = [(i, i + 1) for i in range(n - 1)]
    left = [(i + 1, i) for i in range(n - 1)]

    order = ([0, count - 1] if count > 1 else [0]) + list(range(1, count - 1))
    chunks, sent = [], []
    for t in order:
        free = [
            i
            for i in range(t * tile - margin, (t + 1) * tile + margin, margin)
            if not any(a <= i < b for a, b in sent)
        ]
        chunks.append((free[0], free[-1] + margin))
        sent.append(chunks[-1])

    def pack(jobs):
        return pl.pallas_call(
            functools.partial(pack_kernel, n, tuple((k, chunk[0]) for k, chunk in jobs)),
            out_shape=tuple(VMEM((rows, chunk[1] - chunk[0]), f32) for _, chunk in jobs),
            in_specs=[vm],
            out_specs=(vm,) * len(jobs),
            compiler_params=params(8),
            name="pack",
        )(bands)

    part = min(rows, margin)
    many = margin // part
    outer = [s for s in range(n) if s < many or s >= n - many]

    slots = [[None, *pack([(k, chunks[0]) for k in range(1, n)])]]
    packed = pack([(0, chunks[0])] + [(k, chunk) for chunk in chunks[1:] for k in range(n)])
    slots[0][0] = packed[0]
    slots += [list(packed[i * n + 1 : (i + 1) * n + 1]) for i in range(len(chunks) - 1)]
    rest = []
    for index, got in enumerate(slots):
        late = index > 0 and index == len(slots) - 1
        blocks = list(got)
        for k in range(n - 1, 0, -1):
            pairs = [(i, peer(i, k, n)) for i in range(n)]
            got[k] = lax.ppermute(
                blocks[k], "col", [p for p in pairs if p[0] in outer] if late else pairs
            )
            if late:
                others = [p for p in pairs if p[0] not in outer]
                rest.insert(0, lax.ppermute(blocks[k], "col", others))

    rh, rl = pad_interp(shifted_rows_kernel, row_start, row_interp, (tile, depth))
    ch, cl = pad_interp(shifted_cols_kernel, col_start, col_interp, (count, depth, tile))

    def margins_of(index):
        got = slots[index]
        last, first = pl.pallas_call(
            functools.partial(select_kernel, n, margin),
            out_shape=(VMEM((margin, got[0].shape[1]), f32),) * 2,
            in_specs=[vm] * n,
            out_specs=(vm,) * 2,
            compiler_params=params(8),
            name="select",
        )(*got)
        return lax.ppermute(last, "band", up), lax.ppermute(first, "band", down)

    groups = [[t for t in order if t in (0, count - 1)], [t for t in order if t not in (0, count - 1)]]
    group_of = lambda t: 0 if t in groups[0] else 1
    spans, rr = [], []
    ends = [None, None]
    sides = {}
    tiles = [None] * count

    def run_tile(index, t, margins):
        a0, b0 = chunks[index]
        w = b0 - a0
        spans.append((a0, b0, index))
        parts, olds = [], []
        at, high = t * tile - margin, (t + 1) * tile + margin
        while at < high:
            a, b, which = [s for s in spans if s[0] <= at < s[1]][0]
            end = min(b, high)
            if which == index:
                parts.append(("new", at - a, end - a))
            else:
                if which not in olds:
                    olds.append(which)
                parts.append(("old", olds.index(which), at - a, end - a))
            at = end
        side = [s for s, here in (("first", t == 0), ("last", t == count - 1)) if here]
        doubled = index > 0 and index == len(slots) - 1
        operands = [*slots[index]] + (rest if doubled else [])
        operands += [*margins, rh, rl, ch, cl]
        for which in olds:
            operands += rr[which]
        g = group_of(t)
        place = groups[g].index(t)
        if place:
            operands += ends[g]
        out = pl.pallas_call(
            functools.partial(
                tile_kernel, n, margin, t, tuple(parts), tuple(side), doubled, int(place > 0)
            ),
            out_shape=(
                VMEM((tile, tile), f32),
                VMEM((8, tile * (place + 1)), f32),
                VMEM((8, tile * (place + 1)), f32),
                VMEM((tile, w), bf16),
                VMEM((tile, w), bf16),
            )
            + (VMEM((8, tile), f32),) * len(side),
            in_specs=[vm] * len(operands),
            out_specs=(vm,) * (5 + len(side)),
            scratch_shapes=[VMEM((depth, w), bf16)] * 2,
            compiler_params=params(16),
        )(*operands)
        tiles[t] = out[0]
        ends[g] = (out[1], out[2])
        rr.append((out[3], out[4]))
        for s, v in zip(side, out[5:]):
            sides[s] = v

    def exchange_rows(g):
        heads, tails = ends[g]
        return lax.ppermute(tails, "band", up), lax.ppermute(heads, "band", down)

    def run_horn(ranges, fresh, held):
        some = [t for t in range(count) if tiles[t] is not None][0]
        shown = [tiles[some] if v is None else v for v in tiles]
        scratch = [VMEM((tile, last - first), f32) for first, last in ranges for _ in range(2)]
        return pl.pallas_call(
            functools.partial(horn_kernel, count, tuple(ranges), tuple(fresh), len(held)),
            out_shape=(jax.ShapeDtypeStruct((tile, width), f32),) * 3,
            in_specs=[sm] + [vm] * (count + 2) + [hbm] * len(held),
            out_specs=(hbm,) * 3,
            scratch_shapes=scratch
            + [VMEM((tile, 128), f32)] * 2
            + [
                pltpu.SemaphoreType.DMA((len(fresh),)),
                pltpu.SemaphoreType.DMA((len(ranges), 4, 2)),
            ],
            input_output_aliases={count + 3 + j: j for j in range(len(held))},
            compiler_params=params(16),
        )(spacing, *shown, *lines, *held)

    def make_lines():
        to_left, to_right = pl.pallas_call(
            lines_kernel,
            out_shape=(VMEM((1, tile + 256), f32),) * 2,
            in_specs=[vm] * 4,
            out_specs=(vm,) * 2,
            compiler_params=params(4),
            name="lines",
        )(sides["first"], sides["last"], *halos[0])
        return lax.ppermute(to_right, "col", right), lax.ppermute(to_left, "col", left)

    halos = [None, None]
    lines, maps = None, []
    for index, t in enumerate(order):
        margins = margins_of(index)
        if index > 1 and index == len(order) - 1:
            first, last = t * tile - 128, (t + 1) * tile + 128
            maps = run_horn([(0, first), (last, width)], [i for i in range(count) if i != t], [])
        run_tile(index, t, margins)
        if t == groups[0][-1]:
            halos[0] = exchange_rows(0)
            lines = make_lines()
    if groups[1]:
        halos[1] = exchange_rows(1)
        t = order[-1]
        maps = run_horn([(t * tile - 128, (t + 1) * tile + 128)], [t], list(maps))
    else:
        halos[1] = halos[0]
        maps = run_horn([(0, width)], list(range(count)), [])

    elev, *maps = maps
    where = [(group_of(t), groups[group_of(t)].index(t)) for t in range(count)]
    slope, shade = pl.pallas_call(
        functools.partial(border_kernel, count, tuple(where)),
        out_shape=(jax.ShapeDtypeStruct((tile, width), f32),) * 2,
        in_specs=[sm] + [vm] * (count + 6) + [hbm] * 2,
        out_specs=(hbm,) * 2,
        scratch_shapes=[VMEM((2, 2, 8, width), f32), pltpu.SemaphoreType.DMA((2, 2))],
        input_output_aliases={count + 7: 0, count + 8: 1},
        compiler_params=params(8),
        name="border",
    )(spacing, *tiles, *lines, halos[0][0], halos[1][0], halos[0][1], halos[1][1], *maps)
    return (elev, slope, shade)


def solution(mesh):
    in_specs = (
        P(("band", "col"), None),
        P("band", None, None),
        P("col", None, None),
        P("band"),
        P("col"),
        P("band"),
    )
    out_specs = (P("band", "col"), P("band", "col"), P("band", "col"))

    return jax.shard_map(
        on_device, mesh=mesh, in_specs=in_specs, out_specs=out_specs, check_vma=False
    )
```

```python
import functools

import jax
import jax.numpy as jnp
from jax import lax
from jax.experimental import pallas as pl
from jax.experimental.pallas import tpu as pltpu
from jax.sharding import PartitionSpec as P


MARGIN = 128


VMEM = pltpu.VMEM
SMEM = pltpu.SMEM


def split(x):
    high = x.astype(jnp.bfloat16)
    return high, (x - high.astype(jnp.float32)).astype(jnp.bfloat16)


def dot3(a, b):
    (ah, al), (bh, bl) = a, b
    dot = functools.partial(jnp.dot, preferred_element_type=jnp.float32)
    return dot(ah, bh) + (dot(ah, bl) + dot(al, bh))


def params(mib):
    return pltpu.CompilerParams(vmem_limit_bytes=mib << 20)


def shifted_rows_kernel(start, x_ref, high_ref, low_ref):
    width = high_ref.shape[1]
    x = x_ref[0]
    x = jnp.concatenate([x, jnp.zeros((x.shape[0], width - x.shape[1]), x.dtype)], 1)
    high_ref[...], low_ref[...] = split(pltpu.roll(x, start[0], 1))


def shifted_cols_kernel(start, x_ref, high_ref, low_ref):
    count, depth, tile = high_ref.shape
    for t in range(count):
        x = x_ref[t]
        x = jnp.concatenate([x, jnp.zeros((depth - x.shape[0], tile), x.dtype)], 0)
        high_ref[t], low_ref[t] = split(pltpu.roll(x, start[t], 0))


def pad_interp(kernel, start, x, shape):
    return pl.pallas_call(
        kernel,
        out_shape=(VMEM(shape, jnp.bfloat16),) * 2,
        in_specs=[pl.BlockSpec(memory_space=SMEM), pl.BlockSpec(memory_space=VMEM)],
        out_specs=(pl.BlockSpec(memory_space=VMEM),) * 2,
        compiler_params=params(16),
    )(start, x)


def peer(i, k, n):
    return i ^ k if n & (n - 1) == 0 else (i + k) % n


def source(i, k, n):
    return i ^ k if n & (n - 1) == 0 else (i + n - k) % n


def pack_kernel(n, jobs, bands, *outs):
    me = lax.axis_index("col")
    total = bands.shape[1]
    for (k, first), out in zip(jobs, outs):
        wide = out.shape[1]
        start = jnp.clip(peer(me, k, n) * (total // n) + first, 0, total - wide)
        out[...] = bands[:, pl.ds(pl.multiple_of(start, 128), wide)]


def is_even():
    return lax.axis_index("band") % 2 == 0


def select_kernel(n, margin, extra, *refs):
    slots, refs = refs[:n], refs[n:]
    edges, outs = refs[:extra], refs[extra:]
    me = lax.axis_index("col")
    even = is_even()
    rows = slots[0].shape[0]
    part = min(rows, margin)
    many = margin // part

    def fill(out, to_next):
        first, inner = (n - many, rows - part) if to_next else (0, 0)
        for j in range(many):
            for k in range(n):

                @pl.when(source(me, k, n) == first + j)
                def _():
                    out[j * part : (j + 1) * part, :] = slots[k][inner : inner + part, :]

        for j, edge in enumerate(edges):
            row = 15 if to_next else 0
            out[margin + 8 * j : margin + 8 * j + 8, : edge.shape[1]] = jnp.broadcast_to(
                edge[row : row + 1, :], (8, edge.shape[1])
            )

    for which, out in enumerate(outs):
        pl.when(even == (which == 0))(functools.partial(fill, out, True))
        pl.when(even != (which == 0))(functools.partial(fill, out, False))


def margin_rows(first, second, margin, depth, high, low):
    even = is_even().astype(jnp.int32)
    far = depth - margin
    for x, at in ((first, even * far), (second, (1 - even) * far)):
        spot = pl.ds(pl.multiple_of(at, margin), margin)
        high[spot, :], low[spot, :] = split(x[:margin, :])


def edges_of(z):
    return jnp.concatenate([z[:8], z[z.shape[0] - 8 :]], 0)


def tile_kernel(n, margin, t, side, *refs):
    slots, refs = refs[:n], refs[n:]
    first, second, rh, rl, ch, cl = refs[:6]
    refs = refs[6:]
    z, edges, out_h, out_l, line, high, low = refs[side:]
    me = lax.axis_index("col")
    rows = slots[0].shape[0]
    depth = high.shape[0]
    margin_rows(first, second, margin, depth, high, low)
    for k, slot in enumerate(slots):
        spot = pl.ds(pl.multiple_of(margin + source(me, k, n) * rows, rows), rows)
        high[spot, :], low[spot, :] = split(slot[...])
    rr = dot3((rh[...], rl[...]), (high[...], low[...]))
    none = jnp.zeros((rr.shape[0], margin), rr.dtype)
    if side == 0:
        rr = jnp.where(me == 0, jnp.concatenate([none, rr[:, :-margin]], 1), rr)
    else:
        rr = jnp.where(me == n - 1, jnp.concatenate([rr[:, margin:], none], 1), rr)
    new = split(rr)
    out_h[...], out_l[...] = new
    value = dot3(new, (ch[t], cl[t]))
    z[...] = value
    edges[...] = edges_of(value)
    if side == 0:
        line[...] = value[:, :128].T[:8]
    else:
        line[...] = value[:, value.shape[1] - 128 :].T[120:]
        line[0:1, :] = refs[0][0:1, :]


def inner_partial_kernel(n, margin, spans, *refs):
    slots, refs = refs[:n], refs[n:]
    first, second, rh, rl, ch, cl, ah, al, bh, bl, rr = refs[:11]
    zs, (high, low) = refs[11:-2], refs[-2:]
    me = lax.axis_index("col")
    rows = slots[0].shape[0]
    depth = high.shape[0]
    half = depth // 2
    many = max(margin // rows, 1)
    margin_rows(first, second, margin, depth, high, low)
    for k, slot in enumerate(slots):
        own = source(me, k, n)
        at = jnp.where(own < many, margin + own * rows, depth - margin - (n - own) * rows)

        @pl.when((own < many) | (own >= n - many))
        def _():
            spot = pl.ds(pl.multiple_of(at, rows), rows)
            high[spot, :], low[spot, :] = split(slot[...])

    pick = lambda v: jnp.concatenate([v[:, :half], v[:, v.shape[1] - half :]], 1)
    rr[...] = dot3((pick(rh[...]), pick(rl[...])), (high[...], low[...]))
    for (t, before, fresh, after), z in zip(spans, zs):
        total = jnp.zeros(z.shape, jnp.float32)
        if before:
            wide = ah.shape[1]
            left = (ah[:, wide - before :], al[:, wide - before :])
            total = total + dot3(left, (ch[t, :before, :], cl[t, :before, :]))
        if after:
            right = (bh[:, :after], bl[:, :after])
            total = total + dot3(right, (ch[t, before + fresh :, :], cl[t, before + fresh :, :]))
        z[...] = total


def inner_kernel(n, margin, spans, *refs):
    slots, refs = refs[:n], refs[n:]
    rh, rl, ch, cl, rr, line_a, line_b = refs[:7]
    refs = refs[7:]
    count = len(spans)
    parts, zs, (edges, high, low) = refs[:count], refs[count : 2 * count], refs[2 * count :]
    me = lax.axis_index("col")
    rows = slots[0].shape[0]
    inner = high.shape[0]
    depth = rh.shape[1]
    many = max(margin // rows, 1)
    for k, slot in enumerate(slots):
        own = source(me, k, n)

        @pl.when((own >= many) & (own < n - many))
        def _():
            spot = pl.ds(pl.multiple_of((own - many) * rows, rows), rows)
            high[spot, :], low[spot, :] = split(slot[...])

    low_k = (depth - inner) // 2
    cols = slice(low_k, low_k + inner)
    new = split(rr[...] + dot3((rh[:, cols], rl[:, cols]), (high[...], low[...])))
    tile = zs[0].shape[1]
    for j, ((t, before, fresh, after), part, z) in enumerate(zip(spans, parts, zs)):
        at = max(j * tile - 2 * margin, 0)
        window = tuple(v[:, at : at + fresh] for v in new)
        c = (ch[t, before : before + fresh, :], cl[t, before : before + fresh, :])
        value = part[...] + dot3(window, c)
        z[...] = value
        edges[:, j * tile : (j + 1) * tile] = edges_of(value)
    even = me % 2 == 0
    left = jnp.where(even, line_b[7:8, :], line_a[7:8, :])
    right = jnp.where(even, line_a[0:1, :], line_b[0:1, :])
    wide = count * tile
    for j, v in enumerate((left, right)):
        at = wide + 128 * j
        edges[:8, at : at + 128] = jnp.broadcast_to(v[:, :128], (8, 128))
        edges[8:, at : at + 128] = jnp.broadcast_to(v[:, tile - 128 :], (8, 128))


def across(z):
    width = z.shape[1]
    here = z[:, 128 : width - 128]
    before = pltpu.roll(z, 1, 1)[:, 128 : width - 128]
    after = pltpu.roll(z, width - 1, 1)[:, 128 : width - 128]
    return after - before, before + 2.0 * here + after


def maps_of(p, q, scale):
    p = p * scale
    q = q * scale
    total = p * p + q * q
    inv = lax.rsqrt(1.0 + total)
    root = total * lax.rsqrt(jnp.maximum(total, 1.2e-38))
    return root * inv, (0.70710678 - 0.5 * p + 0.5 * q) * inv


def upright(line, rows):
    return jnp.broadcast_to(line, (128, rows)).T


def cut(tiles, rows, first, last, ends):
    tile = tiles[0].shape[1]
    width = tile * len(tiles)
    pieces = [ends[0]] if first < 0 else []
    at = max(first, 0)
    while at < min(last, width):
        t, stop = at // tile, min(at // tile * tile + tile, last)
        pieces.append(tiles[t][rows, at - t * tile : stop - t * tile])
        at = stop
    if last > width:
        pieces.append(ends[1])
    return jnp.concatenate(pieces, 1)


def horn_kernel(count, ranges, fresh, held, spacing, *refs):
    tiles, (line_a, line_b) = refs[:count], refs[count : count + 2]
    elev, slope, shade, *bufs, l_col, r_col, sem_z, sem_out = refs[count + 2 + held :]
    tile = tiles[0].shape[0]
    width = tile * count
    blocks = 4 if tile % 32 == 0 else 1
    rows = tile // blocks

    def keep(j):
        return pltpu.make_async_copy(
            tiles[fresh[j]], elev.at[:, pl.ds(fresh[j] * tile, tile)], sem_z.at[j]
        )

    def store(i, b, which):
        first, last = ranges[i]
        return pltpu.make_async_copy(
            bufs[2 * i + which].at[pl.ds(b * rows, rows), :],
            (slope, shade)[which].at[pl.ds(b * rows, rows), pl.ds(first, last - first)],
            sem_out.at[i, b, which],
        )

    for j in range(len(fresh)):
        keep(j).start()
    even = lax.axis_index("col") % 2 == 0
    if any(first == 0 for first, _ in ranges):
        l_col[...] = upright(jnp.where(even, line_b[7:8, :], line_a[7:8, :]), tile)
    if any(last == width for _, last in ranges):
        r_col[...] = upright(jnp.where(even, line_a[0:1, :], line_b[0:1, :]), tile)
    strips = tile // 8
    for i, (first, last) in enumerate(ranges):
        pieces, at = [], first
        while at < last:
            pieces.append((at, min(at + 384, last)))
            at = pieces[-1][1]
        for b in range(blocks):
            for lo, hi in pieces:
                row = lax.broadcasted_iota(jnp.int32, (8, hi - lo), 0)
                scale = 0.125 / jnp.full((8, hi - lo), spacing[0])

                def load(g):
                    spot = pl.ds(pl.multiple_of(g * 8, 8), 8)
                    ends = (l_col[spot, :], r_col[spot, :])
                    return across(cut(tiles, spot, lo - 128, hi + 128, ends))

                def rolled(v):
                    return pltpu.roll(v, 1, 0), pltpu.roll(v, 7, 0)

                def strip(r, carry):
                    g = b * (rows // 8) + r
                    e, e1, e7, f1, f7, e1_above, f1_above = carry
                    e_next, f_next = load(jnp.minimum(g + 1, strips - 1))
                    e1_next, e7_next = rolled(e_next)
                    f1_next, f7_next = rolled(f_next)
                    e_up = jnp.where(row == 0, e1_above, e1)
                    f_up = jnp.where(row == 0, f1_above, f1)
                    e_down = jnp.where(row == 7, e7_next, e7)
                    f_down = jnp.where(row == 7, f7_next, f7)
                    spot = pl.ds(pl.multiple_of(g * 8, 8), 8)
                    where = pl.ds(lo - first, hi - lo)
                    bufs[2 * i][spot, where], bufs[2 * i + 1][spot, where] = maps_of(
                        e_up + 2.0 * e + e_down, f_down - f_up, scale
                    )
                    return e_next, e1_next, e7_next, f1_next, f7_next, e1, f1

                g0 = b * (rows // 8)
                e_above, f_above = load(max(g0 - 1, 0))
                e, f = load(g0)
                start = (e, *rolled(e), *rolled(f), rolled(e_above)[0], rolled(f_above)[0])
                lax.fori_loop(0, rows // 8, strip, start, unroll=8)
            store(i, b, 0).start()
            store(i, b, 1).start()
    for i in range(len(ranges)):
        for b in range(blocks):
            store(i, b, 0).wait()
            store(i, b, 1).wait()
    for j in range(len(fresh)):
        keep(j).wait()


def border_kernel(count, margin, spacing, *refs):
    tiles, refs = refs[:count], refs[count:]
    line_a, line_b, outer_a, outer_b, inner_a, inner_b = refs[:6]
    slope, shade, buf, sem = refs[-4:]
    tile = tiles[0].shape[0]
    width = tile * count
    middle = width - 2 * tile
    even = is_even()
    side = lax.axis_index("col") % 2 == 0
    left = jnp.where(side, line_b[7:8, :], line_a[7:8, :])
    right = jnp.where(side, line_a[0:1, :], line_b[0:1, :])
    row = lax.broadcasted_iota(jnp.int32, (8, width), 0)
    scale = 0.125 / jnp.full((8, width), spacing[0])

    def halo(above):
        pick = lambda a, b: jnp.where(even, b, a) if above else jnp.where(even, a, b)
        outer = [
            pick(*(v[margin + 8 * j : margin + 8 * j + 1, :tile] for v in (outer_a, outer_b)))
            for j in range(2)
        ]
        at = 15 if above else 0
        inner = pick(inner_a[at : at + 1, :], inner_b[at : at + 1, :])
        ends = [inner[:, middle : middle + 128], inner[:, middle + 128 :]]
        ends = [jnp.broadcast_to(v, (8, 128)) for v in ends]
        j = 1 if above else 0
        ends[j] = pltpu.roll(ends[j], 1 if above else 127, 1)
        values = jnp.concatenate([outer[0], inner[:, :middle], outer[1]], 1)
        values = jnp.broadcast_to(values, (8, width))
        return across(jnp.concatenate([ends[0], values, ends[1]], 1))

    def strip(at):
        lane = at // 128 * 128
        ends = [upright(v[:, lane : lane + 128], 128)[at - lane : at - lane + 8] for v in (left, right)]
        return across(cut(tiles, slice(at, at + 8), -128, width + 128, ends))

    copies = []
    for where, at in enumerate((0, tile - 8)):
        e, f = strip(at)
        above = halo(True) if where == 0 else [pltpu.roll(v, 1, 0) for v in strip(at - 8)]
        below = halo(False) if where == 1 else [pltpu.roll(v, 7, 0) for v in strip(8)]
        e_up, f_up = [jnp.where(row == 0, a, pltpu.roll(v, 1, 0)) for a, v in zip(above, (e, f))]
        e_down, f_down = [jnp.where(row == 7, a, pltpu.roll(v, 7, 0)) for a, v in zip(below, (e, f))]
        found = maps_of(e_up + 2.0 * e + e_down, f_down - f_up, scale)
        for j, (v, out) in enumerate(zip(found, (slope, shade))):
            buf[where, j] = v
            copies.append(
                pltpu.make_async_copy(buf.at[where, j], out.at[pl.ds(at, 8), :], sem.at[where, j])
            )
            copies[-1].start()
    for copy in copies:
        copy.wait()


def partners(count):
    found = []
    for start in (0, 1):
        pairs = [(i, i + 1) for i in range(start, count - 1, 2)]
        found.append(pairs + [(j, i) for i, j in pairs])
    return found


def on_device(bands, row_interp, col_interp, row_start, col_start, spacing):
    n = lax.axis_size("col")
    nb = lax.axis_size("band")
    margin = MARGIN
    rows, total = bands.shape
    width = total // n
    tile = row_interp.shape[1]
    count = col_interp.shape[0]
    depth = tile + 2 * margin
    f32, bf16 = jnp.float32, jnp.bfloat16
    vm = pl.BlockSpec(memory_space=VMEM)
    sm = pl.BlockSpec(memory_space=SMEM)
    hbm = pl.BlockSpec(memory_space=pltpu.HBM)

    def call(kernel, outs, operands, mib, scratch=()):
        return pl.pallas_call(
            kernel,
            out_shape=tuple(VMEM(shape, dtype) for shape, dtype in outs),
            in_specs=[vm] * len(operands),
            out_specs=(vm,) * len(outs),
            scratch_shapes=scratch,
            compiler_params=params(mib),
        )(*operands)

    def exchange(axis, size, first, second):
        a, b = partners(size)
        return lax.ppermute(first, axis, a), lax.ppermute(second, axis, b)

    chunks = [(-margin, tile + margin), (width - tile - margin, width + margin)]
    chunks.append((tile + margin, width - tile - margin))
    many = max(margin // rows, 1)
    outer = [s for s in range(n) if s < many or s >= n - many]

    def pack(jobs):
        return call(
            functools.partial(pack_kernel, n, tuple((k, chunk[0]) for k, chunk in jobs)),
            [((rows, chunk[1] - chunk[0]), f32) for _, chunk in jobs],
            [bands],
            8,
        )

    blocks = [[None, *pack([(k, chunks[0]) for k in range(1, n)])]]
    packed = pack([(0, chunks[0])] + [(k, chunk) for chunk in chunks[1:] for k in range(n)])
    blocks[0][0] = packed[0]
    blocks += [list(packed[1 : n + 1]), list(packed[n + 1 :])]

    def send(got, keep):
        found = [got[0]]
        for k in range(1, n):
            pairs = [(i, peer(i, k, n)) for i in range(n) if keep(i)]
            found.append(lax.ppermute(got[k], "col", pairs))
        return found

    slots = [send(blocks[i], lambda i: True) for i in range(2)]
    slots.append(send(blocks[2], lambda i: i in outer))
    slots.append(send(blocks[2], lambda i: i not in outer))

    rh, rl = pad_interp(shifted_rows_kernel, row_start, row_interp, (tile, depth))
    ch, cl = pad_interp(shifted_cols_kernel, col_start, col_interp, (count, depth, tile))

    def margins_of(index, edges):
        got = slots[index]
        shape = (margin + 8 * len(edges), got[0].shape[1])
        sent = call(
            functools.partial(select_kernel, n, margin, len(edges)),
            [(shape, f32)] * 2,
            [*got, *edges],
            8,
        )
        return exchange("band", nb, *sent)

    tiles, edges, rr, line = [None] * count, [], [], []
    for side, t in enumerate((0, count - 1)):
        margins = margins_of(side, [])
        wide = chunks[side][1] - chunks[side][0]
        z, edge, high, low, lines = call(
            functools.partial(tile_kernel, n, margin, t, side),
            [((tile, tile), f32), ((16, tile), f32)]
            + [((tile, wide), bf16)] * 2
            + [((8, tile), f32)],
            [*slots[side], *margins, rh, rl, ch, cl, *line],
            16,
            [VMEM((depth, wide), bf16)] * 2,
        )
        tiles[t] = z
        edges.append(edge)
        rr += [high, low]
        line = [lines]
    lines = exchange("col", n, line[0], line[0])

    def run_horn(ranges, fresh, held):
        shown = [tiles[0] if v is None else v for v in tiles]
        scratch = [VMEM((tile, last - first), f32) for first, last in ranges for _ in range(2)]
        return pl.pallas_call(
            functools.partial(horn_kernel, count, tuple(ranges), tuple(fresh), len(held)),
            out_shape=(jax.ShapeDtypeStruct((tile, width), f32),) * 3,
            in_specs=[sm] + [vm] * (count + 2) + [hbm] * len(held),
            out_specs=(hbm,) * 3,
            scratch_shapes=scratch
            + [VMEM((tile, 128), f32)] * 2
            + [
                pltpu.SemaphoreType.DMA((len(fresh),)),
                pltpu.SemaphoreType.DMA((len(ranges), 4, 2)),
            ],
            input_output_aliases={count + 3 + j: j for j in range(len(held))},
            compiler_params=params(16),
        )(spacing, *shown, *lines, *held)

    margins = margins_of(2, edges)
    maps = run_horn([(0, tile - 128), (width - tile + 128, width)], [0, count - 1], [])

    spans = []
    for t in range(1, count - 1):
        low, high = t * tile - margin, (t + 1) * tile + margin
        before, after = max(chunks[2][0] - low, 0), max(high - chunks[2][1], 0)
        spans.append((t, before, depth - before - after, after))
    wide = chunks[2][1] - chunks[2][0]
    part, *partial = call(
        functools.partial(inner_partial_kernel, n, margin, tuple(spans)),
        [((tile, wide), f32)] + [((tile, tile), f32)] * len(spans),
        [*slots[2], *margins, rh, rl, ch, cl, *rr],
        16,
        [VMEM((2 * margin + len(outer) * rows, wide), bf16)] * 2,
    )
    *found, edge = call(
        functools.partial(inner_kernel, n, margin, tuple(spans)),
        [((tile, tile), f32)] * len(spans) + [((16, len(spans) * tile + 256), f32)],
        [*slots[3], rh, rl, ch, cl, part, *lines, *partial],
        16,
        [VMEM(((n - len(outer)) * rows, wide), bf16)] * 2,
    )
    for (t, *_), z in zip(spans, found):
        tiles[t] = z
    ends = exchange("band", nb, edge, edge)
    elev, *maps = run_horn([(tile - 128, width - tile + 128)], [t for t, *_ in spans], list(maps))
    slope, shade = pl.pallas_call(
        functools.partial(border_kernel, count, margin),
        out_shape=(jax.ShapeDtypeStruct((tile, width), f32),) * 2,
        in_specs=[sm] + [vm] * (count + 6) + [hbm] * 2,
        out_specs=(hbm,) * 2,
        scratch_shapes=[VMEM((2, 2, 8, width), f32), pltpu.SemaphoreType.DMA((2, 2))],
        input_output_aliases={count + 7: 0, count + 8: 1},
        compiler_params=params(8),
        name="border",
    )(spacing, *tiles, *lines, *margins, *ends, *maps)
    return (elev, slope, shade)


def solution(mesh):
    in_specs = (
        P(("band", "col"), None),
        P("band", None, None),
        P("col", None, None),
        P("band"),
        P("col"),
        P("band"),
    )
    out_specs = (P("band", "col"), P("band", "col"), P("band", "col"))

    return jax.shard_map(
        on_device, mesh=mesh, in_specs=in_specs, out_specs=out_specs, check_vma=False
    )
```

```python
import functools

import jax
import jax.numpy as jnp
from jax import lax
from jax.experimental import pallas as pl
from jax.experimental.pallas import tpu as pltpu
from jax.sharding import PartitionSpec as P


MARGIN = 128


VMEM = pltpu.VMEM
SMEM = pltpu.SMEM


def split(x):
    high = x.astype(jnp.bfloat16)
    return high, (x - high.astype(jnp.float32)).astype(jnp.bfloat16)


def dot3(a, b):
    (ah, al), (bh, bl) = a, b
    dot = functools.partial(jnp.dot, preferred_element_type=jnp.float32)
    return dot(ah, bh) + (dot(ah, bl) + dot(al, bh))


def params(mib):
    return pltpu.CompilerParams(vmem_limit_bytes=mib << 20)


def shifted_rows_kernel(start, x_ref, high_ref, low_ref):
    width = high_ref.shape[1]
    x = x_ref[0]
    x = jnp.concatenate([x, jnp.zeros((x.shape[0], width - x.shape[1]), x.dtype)], 1)
    high_ref[...], low_ref[...] = split(pltpu.roll(x, start[0], 1))


def shifted_cols_kernel(start, x_ref, high_ref, low_ref):
    count, depth, tile = high_ref.shape
    for t in range(count):
        x = x_ref[t]
        x = jnp.concatenate([x, jnp.zeros((depth - x.shape[0], tile), x.dtype)], 0)
        high_ref[t], low_ref[t] = split(pltpu.roll(x, start[t], 0))


def pad_interp(kernel, start, x, shape):
    return pl.pallas_call(
        kernel,
        out_shape=(VMEM(shape, jnp.bfloat16),) * 2,
        in_specs=[pl.BlockSpec(memory_space=SMEM), pl.BlockSpec(memory_space=VMEM)],
        out_specs=(pl.BlockSpec(memory_space=VMEM),) * 2,
        compiler_params=params(16),
    )(start, x)


def peer(i, k, n):
    return i ^ k if n & (n - 1) == 0 else (i + k) % n


def source(i, k, n):
    return i ^ k if n & (n - 1) == 0 else (i + n - k) % n


def pack_kernel(n, jobs, bands, *outs):
    me = lax.axis_index("col")
    total = bands.shape[1]
    for (k, first), out in zip(jobs, outs):
        wide = out.shape[1]
        start = jnp.clip(peer(me, k, n) * (total // n) + first, 0, total - wide)
        out[...] = bands[:, pl.ds(pl.multiple_of(start, 128), wide)]


def is_even():
    return lax.axis_index("band") % 2 == 0


def select_kernel(n, margin, *refs):
    slots, outs = refs[:n], refs[n:]
    me = lax.axis_index("col")
    even = is_even()
    rows = slots[0].shape[0]
    part = min(rows, margin)
    many = margin // part

    def fill(out, to_next):
        first, inner = (n - many, rows - part) if to_next else (0, 0)
        for j in range(many):
            for k in range(n):

                @pl.when(source(me, k, n) == first + j)
                def _():
                    out[j * part : (j + 1) * part, :] = slots[k][inner : inner + part, :]

    for which, out in enumerate(outs):
        pl.when(even == (which == 0))(functools.partial(fill, out, True))
        pl.when(even != (which == 0))(functools.partial(fill, out, False))


def margin_rows(first, second, margin, depth, high, low):
    even = is_even().astype(jnp.int32)
    far = depth - margin
    for x, at in ((first, even * far), (second, (1 - even) * far)):
        spot = pl.ds(pl.multiple_of(at, margin), margin)
        high[spot, :], low[spot, :] = split(x[...])


def edges_of(z):
    return jnp.concatenate([z[:8], z[z.shape[0] - 8 :]], 0)


def tile_kernel(n, margin, t, side, *refs):
    slots, refs = refs[:n], refs[n:]
    first, second, rh, rl, ch, cl = refs[:6]
    refs = refs[6:]
    z, edges, out_h, out_l, line, high, low = refs[side:]
    me = lax.axis_index("col")
    rows = slots[0].shape[0]
    depth = high.shape[0]
    margin_rows(first, second, margin, depth, high, low)
    for k, slot in enumerate(slots):
        spot = pl.ds(pl.multiple_of(margin + source(me, k, n) * rows, rows), rows)
        high[spot, :], low[spot, :] = split(slot[...])
    rr = dot3((rh[...], rl[...]), (high[...], low[...]))
    none = jnp.zeros((rr.shape[0], margin), rr.dtype)
    if side == 0:
        rr = jnp.where(me == 0, jnp.concatenate([none, rr[:, :-margin]], 1), rr)
    else:
        rr = jnp.where(me == n - 1, jnp.concatenate([rr[:, margin:], none], 1), rr)
    new = split(rr)
    out_h[...], out_l[...] = new
    at = side * (rr.shape[1] - depth)
    value = dot3(tuple(v[:, at : at + depth] for v in new), (ch[t], cl[t]))
    z[...] = value
    edges[...] = edges_of(value)
    if side == 0:
        line[...] = value[:, :128].T[:8]
    else:
        line[...] = value[:, value.shape[1] - 128 :].T[120:]
        line[0:1, :] = refs[0][0:1, :]


def inner_partial_kernel(n, margin, spans, *refs):
    slots, refs = refs[:n], refs[n:]
    rh, rl, ch, cl, ah, al, bh, bl, rr = refs[:9]
    zs, (high, low) = refs[9:-2], refs[-2:]
    me = lax.axis_index("col")
    rows = slots[0].shape[0]
    depth = rh.shape[1]
    for k, slot in enumerate(slots):
        spot = pl.ds(pl.multiple_of(source(me, k, n) * rows, rows), rows)
        high[spot, :], low[spot, :] = split(slot[...])
    own = slice(margin, depth - margin)
    rr[...] = dot3((rh[:, own], rl[:, own]), (high[...], low[...]))
    for (t, _, before, fresh, after), z in zip(spans, zs):
        total = jnp.zeros(z.shape, jnp.float32)
        if before:
            wide = ah.shape[1]
            left = (ah[:, wide - before :], al[:, wide - before :])
            total = total + dot3(left, (ch[t, :before, :], cl[t, :before, :]))
        if after:
            right = (bh[:, :after], bl[:, :after])
            total = total + dot3(right, (ch[t, before + fresh :, :], cl[t, before + fresh :, :]))
        z[...] = total


def inner_kernel(margin, spans, *refs):
    first, second, rh, rl, ch, cl, rr, line_a, line_b, first_edges, last_edges = refs[:11]
    refs = refs[11:]
    count = len(spans)
    parts, zs, (edges, high, low) = refs[:count], refs[count : 2 * count], refs[2 * count :]
    me = lax.axis_index("col")
    depth = rh.shape[1]
    margin_rows(first, second, margin, 2 * margin, high, low)
    ends = lambda v: jnp.concatenate([v[:, :margin], v[:, depth - margin :]], 1)
    new = split(rr[...] + dot3((ends(rh), ends(rl)), (high[...], low[...])))
    tile = zs[0].shape[1]
    for (t, at, before, fresh, after), part, z in zip(spans, parts, zs):
        window = tuple(v[:, at : at + fresh] for v in new)
        c = (ch[t, before : before + fresh, :], cl[t, before : before + fresh, :])
        value = part[...] + dot3(window, c)
        z[...] = value
        edges[:, t * tile : (t + 1) * tile] = edges_of(value)
    edges[:, :tile] = first_edges[...]
    wide = (count + 2) * tile
    edges[:, wide - tile : wide] = last_edges[...]
    even = me % 2 == 0
    left = jnp.where(even, line_b[7:8, :], line_a[7:8, :])
    right = jnp.where(even, line_a[0:1, :], line_b[0:1, :])
    edges[:, :tile] = first_edges[...]
    wide = (count + 2) * tile
    edges[:, wide - tile : wide] = last_edges[...]
    for j, v in enumerate((left, right)):
        at = wide + 128 * j
        edges[:8, at : at + 128] = jnp.broadcast_to(v[:, :128], (8, 128))
        edges[8:, at : at + 128] = jnp.broadcast_to(v[:, tile - 128 :], (8, 128))


def across(z):
    width = z.shape[1]
    here = z[:, 128 : width - 128]
    before = pltpu.roll(z, 1, 1)[:, 128 : width - 128]
    after = pltpu.roll(z, width - 1, 1)[:, 128 : width - 128]
    return after - before, before + 2.0 * here + after


def scales(spacing, shape):
    scale = 0.125 / jnp.full(shape, spacing[0])
    return scale * scale, 0.5 * scale


def maps_of(p, q, factors):
    square, half = factors
    total = (p * p + q * q) * square
    inv = lax.rsqrt(1.0 + total)
    root = total * lax.rsqrt(jnp.maximum(total, 1.2e-38))
    return root * inv, (0.70710678 + (q - p) * half) * inv


def upright(line, rows):
    return jnp.broadcast_to(line, (128, rows)).T


def cut(tiles, rows, first, last, ends):
    tile = tiles[0].shape[1]
    width = tile * len(tiles)
    pieces = [ends[0]] if first < 0 else []
    at = max(first, 0)
    while at < min(last, width):
        t, stop = at // tile, min(at // tile * tile + tile, last)
        pieces.append(tiles[t][rows, at - t * tile : stop - t * tile])
        at = stop
    if last > width:
        pieces.append(ends[1])
    return jnp.concatenate(pieces, 1)


def horn_kernel(count, ranges, fresh, held, spacing, *refs):
    tiles, (line_a, line_b) = refs[:count], refs[count : count + 2]
    elev, slope, shade, *bufs, l_col, r_col, sem_z, sem_out = refs[count + 2 + held :]
    tile = tiles[0].shape[0]
    width = tile * count
    blocks = 4 if tile % 32 == 0 else 1
    rows = tile // blocks

    def keep(j):
        return pltpu.make_async_copy(
            tiles[fresh[j]], elev.at[:, pl.ds(fresh[j] * tile, tile)], sem_z.at[j]
        )

    def store(i, b, which):
        first, last = ranges[i]
        return pltpu.make_async_copy(
            bufs[2 * i + which].at[pl.ds(b * rows, rows), :],
            (slope, shade)[which].at[pl.ds(b * rows, rows), pl.ds(first, last - first)],
            sem_out.at[i, b, which],
        )

    for j in range(len(fresh)):
        keep(j).start()
    even = lax.axis_index("col") % 2 == 0
    if any(first == 0 for first, _ in ranges):
        l_col[...] = upright(jnp.where(even, line_b[7:8, :], line_a[7:8, :]), tile)
    if any(last == width for _, last in ranges):
        r_col[...] = upright(jnp.where(even, line_a[0:1, :], line_b[0:1, :]), tile)
    strips = tile // 8
    for i, (first, last) in enumerate(ranges):
        pieces, at = [], first
        while at < last:
            pieces.append((at, min(at + 640, last)))
            at = pieces[-1][1]
        for b in range(blocks):
            for lo, hi in pieces:
                row = lax.broadcasted_iota(jnp.int32, (8, hi - lo), 0)
                scale = scales(spacing, (8, hi - lo))

                def load(g):
                    spot = pl.ds(pl.multiple_of(g * 8, 8), 8)
                    ends = (l_col[spot, :], r_col[spot, :])
                    return across(cut(tiles, spot, lo - 128, hi + 128, ends))

                def rolled(v):
                    return pltpu.roll(v, 1, 0), pltpu.roll(v, 7, 0)

                def strip(r, carry):
                    g = b * (rows // 8) + r
                    e, e1, e7, f1, f7, e1_above, f1_above = carry
                    e_next, f_next = load(jnp.minimum(g + 1, strips - 1))
                    e1_next, e7_next = rolled(e_next)
                    f1_next, f7_next = rolled(f_next)
                    e_up = jnp.where(row == 0, e1_above, e1)
                    f_up = jnp.where(row == 0, f1_above, f1)
                    e_down = jnp.where(row == 7, e7_next, e7)
                    f_down = jnp.where(row == 7, f7_next, f7)
                    spot = pl.ds(pl.multiple_of(g * 8, 8), 8)
                    where = pl.ds(lo - first, hi - lo)
                    bufs[2 * i][spot, where], bufs[2 * i + 1][spot, where] = maps_of(
                        e_up + 2.0 * e + e_down, f_down - f_up, scale
                    )
                    return e_next, e1_next, e7_next, f1_next, f7_next, e1, f1

                g0 = b * (rows // 8)
                e_above, f_above = load(max(g0 - 1, 0))
                e, f = load(g0)
                start = (e, *rolled(e), *rolled(f), rolled(e_above)[0], rolled(f_above)[0])
                lax.fori_loop(0, rows // 8, strip, start, unroll=rows // 8)
            store(i, b, 0).start()
            store(i, b, 1).start()
    for i in range(len(ranges)):
        for b in range(blocks):
            store(i, b, 0).wait()
            store(i, b, 1).wait()
    for j in range(len(fresh)):
        keep(j).wait()


def border_kernel(count, spacing, *refs):
    tiles, refs = refs[:count], refs[count:]
    line_a, line_b, edges_a, edges_b = refs[:4]
    slope, shade, buf, sem = refs[-4:]
    tile = tiles[0].shape[0]
    width = tile * count
    even = is_even()
    side = lax.axis_index("col") % 2 == 0
    left = jnp.where(side, line_b[7:8, :], line_a[7:8, :])
    right = jnp.where(side, line_a[0:1, :], line_b[0:1, :])
    row = lax.broadcasted_iota(jnp.int32, (8, width), 0)
    scale = scales(spacing, (8, width))

    def halo(above):
        at = 15 if above else 0
        a, b = edges_a[at : at + 1, :], edges_b[at : at + 1, :]
        found = jnp.where(even, b, a) if above else jnp.where(even, a, b)
        ends = [found[:, width : width + 128], found[:, width + 128 :]]
        ends = [jnp.broadcast_to(v, (8, 128)) for v in ends]
        j = 1 if above else 0
        ends[j] = pltpu.roll(ends[j], 1 if above else 127, 1)
        values = jnp.broadcast_to(found[:, :width], (8, width))
        return across(jnp.concatenate([ends[0], values, ends[1]], 1))

    def strip(at):
        lane = at // 128 * 128
        ends = [upright(v[:, lane : lane + 128], 128)[at - lane : at - lane + 8] for v in (left, right)]
        return across(cut(tiles, slice(at, at + 8), -128, width + 128, ends))

    copies = []
    for where, at in enumerate((0, tile - 8)):
        e, f = strip(at)
        above = halo(True) if where == 0 else [pltpu.roll(v, 1, 0) for v in strip(at - 8)]
        below = halo(False) if where == 1 else [pltpu.roll(v, 7, 0) for v in strip(8)]
        e_up, f_up = [jnp.where(row == 0, a, pltpu.roll(v, 1, 0)) for a, v in zip(above, (e, f))]
        e_down, f_down = [jnp.where(row == 7, a, pltpu.roll(v, 7, 0)) for a, v in zip(below, (e, f))]
        found = maps_of(e_up + 2.0 * e + e_down, f_down - f_up, scale)
        for j, (v, out) in enumerate(zip(found, (slope, shade))):
            buf[where, j] = v
            copies.append(
                pltpu.make_async_copy(buf.at[where, j], out.at[pl.ds(at, 8), :], sem.at[where, j])
            )
            copies[-1].start()
    for copy in copies:
        copy.wait()


def partners(count):
    found = []
    for start in (0, 1):
        pairs = [(i, i + 1) for i in range(start, count - 1, 2)]
        found.append(pairs + [(j, i) for i, j in pairs])
    return found


def on_device(bands, row_interp, col_interp, row_start, col_start, spacing):
    n = lax.axis_size("col")
    nb = lax.axis_size("band")
    margin = MARGIN
    rows, total = bands.shape
    width = total // n
    tile = row_interp.shape[1]
    count = col_interp.shape[0]
    depth = tile + 2 * margin
    f32, bf16 = jnp.float32, jnp.bfloat16
    vm = pl.BlockSpec(memory_space=VMEM)
    sm = pl.BlockSpec(memory_space=SMEM)
    hbm = pl.BlockSpec(memory_space=pltpu.HBM)

    def call(kernel, outs, operands, mib, scratch=()):
        return pl.pallas_call(
            kernel,
            out_shape=tuple(VMEM(shape, dtype) for shape, dtype in outs),
            in_specs=[vm] * len(operands),
            out_specs=(vm,) * len(outs),
            scratch_shapes=scratch,
            compiler_params=params(mib),
        )(*operands)

    def exchange(axis, size, first, second):
        a, b = partners(size)
        return lax.ppermute(first, axis, a), lax.ppermute(second, axis, b)

    more = 2 * margin if width - 2 * tile > 4 * margin else 0
    ends = (tile + margin + more, width - tile - margin)
    chunks = [(-margin, ends[0]), (ends[1], width + margin), ends]

    def pack(jobs):
        return call(
            functools.partial(pack_kernel, n, tuple((k, chunk[0]) for k, chunk in jobs)),
            [((rows, chunk[1] - chunk[0]), f32) for _, chunk in jobs],
            [bands],
            8,
        )

    blocks = [[None, *pack([(k, chunks[0]) for k in range(1, n)])]]
    packed = pack([(0, chunks[0])] + [(k, chunk) for chunk in chunks[1:] for k in range(n)])
    blocks[0][0] = packed[0]
    blocks += [list(packed[1 : n + 1]), list(packed[n + 1 :])]

    def send(got):
        found = [got[0]]
        for k in range(1, n):
            pairs = [(i, peer(i, k, n)) for i in range(n)]
            found.append(lax.ppermute(got[k], "col", pairs))
        return found

    slots = [send(got) for got in blocks]

    rh, rl = pad_interp(shifted_rows_kernel, row_start, row_interp, (tile, depth))
    ch, cl = pad_interp(shifted_cols_kernel, col_start, col_interp, (count, depth, tile))

    def margins_of(index):
        got = slots[index]
        shape = (margin, got[0].shape[1])
        sent = call(functools.partial(select_kernel, n, margin), [(shape, f32)] * 2, got, 8)
        return exchange("band", nb, *sent)

    tiles, edges, rr, line = [None] * count, [], [], []
    for side, t in enumerate((0, count - 1)):
        margins = margins_of(side)
        wide = chunks[side][1] - chunks[side][0]
        z, edge, high, low, lines = call(
            functools.partial(tile_kernel, n, margin, t, side),
            [((tile, tile), f32), ((16, tile), f32)]
            + [((tile, wide), bf16)] * 2
            + [((8, tile), f32)],
            [*slots[side], *margins, rh, rl, ch, cl, *line],
            16,
            [VMEM((depth, wide), bf16)] * 2,
        )
        tiles[t] = z
        edges.append(edge)
        rr += [high, low]
        line = [lines]
    lines = exchange("col", n, line[0], line[0])

    def run_horn(ranges, fresh, held):
        shown = [tiles[0] if v is None else v for v in tiles]
        scratch = [VMEM((tile, last - first), f32) for first, last in ranges for _ in range(2)]
        return pl.pallas_call(
            functools.partial(horn_kernel, count, tuple(ranges), tuple(fresh), len(held)),
            out_shape=(jax.ShapeDtypeStruct((tile, width), f32),) * 3,
            in_specs=[sm] + [vm] * (count + 2) + [hbm] * len(held),
            out_specs=(hbm,) * 3,
            scratch_shapes=scratch
            + [VMEM((tile, 128), f32)] * 2
            + [
                pltpu.SemaphoreType.DMA((len(fresh),)),
                pltpu.SemaphoreType.DMA((len(ranges), 4, 2)),
            ],
            input_output_aliases={count + 3 + j: j for j in range(len(held))},
            compiler_params=params(16),
        )(spacing, *shown, *lines, *held)

    margins = margins_of(2)
    maps = run_horn([(0, tile - 128), (width - tile + 128, width)], [0, count - 1], [])

    spans = []
    for t in range(1, count - 1):
        low, high = t * tile - margin, (t + 1) * tile + margin
        before, after = max(chunks[2][0] - low, 0), max(high - chunks[2][1], 0)
        spans.append((t, max(low - chunks[2][0], 0), before, depth - before - after, after))
    wide = chunks[2][1] - chunks[2][0]
    part, *partial = call(
        functools.partial(inner_partial_kernel, n, margin, tuple(spans)),
        [((tile, wide), f32)] + [((tile, tile), f32)] * len(spans),
        [*slots[2], rh, rl, ch, cl, *rr],
        16,
        [VMEM((n * rows, wide), bf16)] * 2,
    )
    *found, edge = call(
        functools.partial(inner_kernel, margin, tuple(spans)),
        [((tile, tile), f32)] * len(spans) + [((16, width + 256), f32)],
        [*margins, rh, rl, ch, cl, part, *lines, *edges, *partial],
        16,
        [VMEM((2 * margin, wide), bf16)] * 2,
    )
    for (t, *_), z in zip(spans, found):
        tiles[t] = z
    ends = exchange("band", nb, edge, edge)
    elev, *maps = run_horn([(tile - 128, width - tile + 128)], [t for t, *_ in spans], list(maps))
    slope, shade = pl.pallas_call(
        functools.partial(border_kernel, count),
        out_shape=(jax.ShapeDtypeStruct((tile, width), f32),) * 2,
        in_specs=[sm] + [vm] * (count + 4) + [hbm] * 2,
        out_specs=(hbm,) * 2,
        scratch_shapes=[VMEM((2, 2, 8, width), f32), pltpu.SemaphoreType.DMA((2, 2))],
        input_output_aliases={count + 5: 0, count + 6: 1},
        compiler_params=params(8),
        name="border",
    )(spacing, *tiles, *lines, *ends, *maps)
    return (elev, slope, shade)


def solution(mesh):
    in_specs = (
        P(("band", "col"), None),
        P("band", None, None),
        P("col", None, None),
        P("band"),
        P("col"),
        P("band"),
    )
    out_specs = (P("band", "col"), P("band", "col"), P("band", "col"))

    return jax.shard_map(
        on_device, mesh=mesh, in_specs=in_specs, out_specs=out_specs, check_vma=False
    )
```
